64 devices in a mesh: data: 4 (over x, y), dap: 16 (over z, core).
Axes of the slice: x: 2, y: 2, z: 8, core: 2. Of those that a mesh axis runs over, the one named last changes fastest.
The devices are a block of a 4x4x8 slice.
Arguments:
- z: bfloat16 [1024, 256, 128], P(('data', 'dap')), parts along dimension 0
- res_mask: int32 [1024], P('data'), parts along dimension 0
- ln_w: bfloat16 [8, 2, 2, 128], replicated
- w_in: bfloat16 [8, 2, 128, 512], replicated
- b_g: bfloat16 [8, 2, 128], replicated
- w_b: bfloat16 [8, 2, 128, 4], replicated
- w_o: bfloat16 [8, 2, 128, 128], replicated
- b_o: bfloat16 [8, 2, 128], replicated
Outputs:
- output: bfloat16 [1024, 256, 128], P(('data', 'dap')), parts along dimension 0
There are 4 independent parts. The reference program is written for one: setup_inputs(seed, part) draws one part's arguments, and reference() takes and returns one part's arrays. A program takes and returns all parts, laid end to end along the dimension named above; an argument that names none is the same for every part.
All inputs are finite; a program needn't handle non-finite values.
Results may differ from the reference program's by a relative error of at most 0.02.
Values are sent between devices in bfloat16 or wider.
A program may use at most 768 MiB of HBM per device.

```python
import jax
import jax.numpy as jnp
from jax import lax

NR = 256
C_Z = 128
HEADS = 4
HEAD = 32
LAYERS = 8

EPS = 1e-5
NEG = -1e9


def setup_inputs(seed: int = 0, part: int = 0) -> dict:
    key = jax.random.PRNGKey(seed)
    kz, km = jax.random.split(jax.random.fold_in(jax.random.fold_in(key, 1), part))
    kw = jax.random.split(jax.random.fold_in(key, 0), 7)
    hd = HEADS * HEAD
    z = jax.random.normal(kz, (NR, NR, C_Z), jnp.float32)
    keep = jax.random.uniform(km, (NR,), jnp.float32) > 0.2
    res_mask = jnp.where(jnp.arange(NR) == 0, True, keep).astype(jnp.int32)
    gamma = 1.0 + 0.1 * jax.random.normal(kw[0], (LAYERS, 2, 1, C_Z), jnp.float32)
    beta = 0.1 * jax.random.normal(kw[1], (LAYERS, 2, 1, C_Z), jnp.float32)
    w_in = jax.random.normal(kw[2], (LAYERS, 2, C_Z, 4 * hd), jnp.float32) * C_Z ** -0.5
    b_g = 0.5 * jax.random.normal(kw[3], (LAYERS, 2, hd), jnp.float32)
    w_b = 1.5 * jax.random.normal(kw[4], (LAYERS, 2, C_Z, HEADS), jnp.float32) * C_Z ** -0.5
    w_o = jax.random.normal(kw[5], (LAYERS, 2, hd, C_Z), jnp.float32) * hd ** -0.5
    b_o = 0.1 * jax.random.normal(kw[6], (LAYERS, 2, C_Z), jnp.float32)
    bf = jnp.bfloat16
    return {'z': z.astype(bf), 'res_mask': res_mask,
            'ln_w': jnp.concatenate([gamma, beta], axis=2).astype(bf),
            'w_in': w_in.astype(bf), 'b_g': b_g.astype(bf), 'w_b': w_b.astype(bf),
            'w_o': w_o.astype(bf), 'b_o': b_o.astype(bf)}


def _ln(x, w):
    x = x.astype(jnp.float32)
    mu = jnp.mean(x, axis=-1, keepdims=True)
    var = jnp.mean(jnp.square(x - mu), axis=-1, keepdims=True)
    y = (x - mu) * lax.rsqrt(var + EPS)
    return (y * w[0].astype(jnp.float32) + w[1].astype(jnp.float32)).astype(jnp.bfloat16)


def _tri_start(z, res_mask, ln_w, w_in, b_g, w_b, w_o, b_o):
    def pair_bias(zr):
        return jnp.dot(_ln(zr, ln_w), w_b, preferred_element_type=jnp.float32).astype(jnp.bfloat16)
    b = lax.map(pair_bias, z)
    mask_bias = jnp.where(res_mask > 0, 0.0, NEG)
    bias = jnp.transpose(b, (2, 0, 1)).astype(jnp.float32) + mask_bias[None, None, :]
    gate_b = b_g.astype(jnp.float32).reshape(HEADS, HEAD)

    def row(zr):
        y = _ln(zr, ln_w)
        proj = jnp.dot(y, w_in, preferred_element_type=jnp.float32).reshape(NR, 4, HEADS, HEAD)
        q = proj[:, 0].astype(jnp.bfloat16)
        k = proj[:, 1].astype(jnp.bfloat16)
        v = proj[:, 2].astype(jnp.bfloat16)
        g = jax.nn.sigmoid(proj[:, 3] + gate_b)
        s = jnp.einsum('jhd,khd->hjk', q.astype(jnp.float32), k.astype(jnp.float32)) * HEAD ** -0.5 + bias
        p = jax.nn.softmax(s, axis=-1).astype(jnp.bfloat16)
        o = jnp.einsum('hjk,khd->jhd', p.astype(jnp.float32), v.astype(jnp.float32))
        o = (g * o).astype(jnp.bfloat16).reshape(NR, HEADS * HEAD)
        upd = jnp.dot(o, w_o, preferred_element_type=jnp.float32) + b_o.astype(jnp.float32)
        return (zr.astype(jnp.float32) + upd).astype(jnp.bfloat16)

    return lax.map(row, z)


def reference(z, res_mask, ln_w, w_in, b_g, w_b, w_o, b_o):
    def layer(z, w):
        lw, wi, bg, wb, wo, bo = w
        z = _tri_start(z, res_mask, lw[0], wi[0], bg[0], wb[0], wo[0], bo[0])
        zt = _tri_start(jnp.swapaxes(z, 0, 1), res_mask, lw[1], wi[1], bg[1], wb[1], wo[1], bo[1])
        return jnp.swapaxes(zt, 0, 1), None
    z, _ = lax.scan(layer, z, (ln_w, w_in, b_g, w_b, w_o, b_o))
    return z
```

```python
import functools
import math

import jax
import jax.numpy as jnp
from jax import lax
from jax.experimental import pallas as pl
from jax.experimental.pallas import tpu as pltpu
from jax.sharding import PartitionSpec as P

EPS = 1e-5
NEG = -1e9
LOG2E = math.log2(math.e)
F32 = jnp.float32
BF16 = jnp.bfloat16
MESH = pl.DeviceIdType.MESH
LANES = 128
ROWS = 4


def _ln(x, w):
    mu = jnp.mean(x, axis=-1, keepdims=True)
    xc = x - mu
    var = jnp.mean(xc * xc, axis=-1, keepdims=True)
    return (xc * lax.rsqrt(var + EPS) * w[0:1] + w[1:2]).astype(BF16)


def _nt(a, b):
    return lax.dot_general(a, b, (((1,), (1,)), ((), ())), preferred_element_type=F32)


def _tn(a, b):
    return lax.dot_general(a, b, (((0,), (0,)), ((), ())), preferred_element_type=F32)


def _dot(a, b):
    return jnp.dot(a, b, preferred_element_type=F32)


def _kernel(nd, nm, zin, maskb, lnw, wk, wt, bg, wb, wo, bo, out,
            zout, bout, zbuf, bbuf, zf, bf, bias, mbuf,
            zs, bs, zr, br, ms, mr):
    r, n, c = zin.shape
    passes, hd = wk.shape[0], wk.shape[2]
    heads = wb.shape[1] // 2
    d = hd // heads
    last = passes - 1
    scale = d ** -0.5 * LOG2E

    me_d, me_p = lax.axis_index("data"), lax.axis_index("dap")
    side = math.isqrt(nd)
    cube = side * side == nd and side % 2 == 0 and nm % 4 == 0
    if cube:
        sub = nm // 4
        x, y = me_d // side, me_d % side
        x0, y0 = x - x % 2, y - y % 2
        low = (x % 2) * 2 + y % 2
        mine = me_p // sub
        slot = low * sub + me_p % sub

        def home_of(crop, u):
            return (x0 + crop // 2) * side + y0 + crop % 2, u

        def cube_of(crop, u):
            lo = u // sub
            return (x0 + lo // 2) * side + y0 + lo % 2, crop * sub + u % sub
    else:
        low, mine, slot = me_d, me_d, me_p

        def home_of(crop, u):
            return me_d, u

        cube_of = home_of

    def is_me(t):
        return jnp.logical_and(t[0] == me_d, t[1] == me_p)

    def shifted(base, s):
        return (base + s) % nm

    inside = (low == mine) if cube else True

    def send(src, dst, ss, rs, target, kind, s):
        def local():
            pltpu.make_async_copy(src, dst, rs).start()

        def remote():
            pltpu.make_async_remote_copy(src, dst, ss, rs, device_id=target, device_id_type=MESH).start()

        if kind == "mid" or not cube:
            (local if s == 0 else remote)()
        else:
            me = is_me(target)
            pl.when(me)(local)
            pl.when(jnp.logical_not(me))(remote)

    def drain(ref, sem):
        pltpu.make_async_copy(ref, ref, sem).wait()

    def drain_sent(ref_all, ref_less, sem, kind):
        if kind == "mid" or not cube:
            drain(ref_less, sem)
        else:
            pl.when(inside)(lambda: drain(ref_less, sem))
            pl.when(jnp.logical_not(inside))(lambda: drain(ref_all, sem))

    barrier = pltpu.get_barrier_semaphore()
    groups = [(home_of, low), (cube_of, mine)] + ([(cube_of, low), (home_of, mine)] if cube else [])
    if not cube:
        groups = groups[:1]
    for of, crop in groups:
        def greet(u, carry, of=of, crop=crop):
            t = of(crop, u)

            @pl.when(jnp.logical_not(is_me(t)))
            def _():
                pl.semaphore_signal(barrier, inc=1, device_id=t, device_id_type=MESH)
            return carry
        lax.fori_loop(0, nm, greet, 0)
    if cube:
        @pl.when(inside)
        def _():
            pl.semaphore_wait(barrier, 4 * (nm - 1))

        @pl.when(jnp.logical_not(inside))
        def _():
            pl.semaphore_wait(barrier, 2 * (nm - 1) + 2 * nm)
    else:
        pl.semaphore_wait(barrier, nm - 1)

    low_half = lax.broadcasted_iota(jnp.int32, (2 * heads, LANES), 0) < heads

    def bias_rows(z, w, wbw):
        b = _nt(wbw, _ln(z, w))
        return jnp.where(low_half, b[:, :LANES], b[:, LANES:]).astype(BF16)

    mbuf[0] = maskb[...]
    mt = cube_of(low, me_p)
    if cube:
        me_m = is_me(mt)
        pl.when(me_m)(lambda: pltpu.make_async_copy(maskb, mbuf.at[1], mr).start())
        pl.when(jnp.logical_not(me_m))(lambda: pltpu.make_async_remote_copy(
            maskb, mbuf.at[1], ms, mr, device_id=mt, device_id_type=MESH).start())
    else:
        pltpu.make_async_copy(maskb, mbuf.at[1], mr).start()

    def first_bias(i, carry):
        w = lnw[0]
        for q in range(ROWS):
            row = i * ROWS + q
            bout[row] = bias_rows(zin[row].astype(F32), w, wb[0])
        return carry
    lax.fori_loop(0, r // ROWS, first_bias, 0)
    for s in range(nm):
        u = shifted(me_p, s)
        send(bout, bbuf.at[2, pl.ds(me_p * r, r)], bs, br.at[2], home_of(low, u), "mid", s)
    drain(bbuf.at[2], br.at[2])
    drain(bbuf.at[2, pl.ds(0, n - r)], bs)
    if cube:
        pl.when(jnp.logical_not(me_m))(lambda: drain(maskb, ms))
    drain(mbuf.at[1], mr)

    def run_pass(p, kind):
        now = 2 if kind == "first" else p % 2
        later = 2 if kind == "last" else (p + 1) % 2
        if kind != "first":
            drain(zbuf.at[now], zr.at[now])
            drain(bbuf.at[now], br.at[now])

            def widen(i, carry):
                rows = pl.ds(pl.multiple_of(i * r * r, r * r), r * r)
                zf[rows, :] = zbuf[now, pl.ds(i * r, r)].astype(F32).reshape(r * r, c)
                return carry
            lax.fori_loop(0, n // r, widen, 0)

        def widen_bias(i, carry):
            rows = pl.ds(pl.multiple_of(i * r * 2 * heads, r * 2 * heads), r * 2 * heads)
            bf[rows, :] = bbuf[now, pl.ds(i * r, r)].astype(F32).reshape(r * 2 * heads, LANES)
            return carry
        lax.fori_loop(0, n // r, widen_bias, 0)
        mask = mbuf.at[0 if kind == "first" else 1]
        for h in range(heads):
            halves = [bf[pl.ds(half * heads + h, n, stride=2 * heads), :] * LOG2E for half in range(2)]
            if kind == "first":
                halves = jnp.split(jnp.concatenate(halves, axis=1).T, 2, axis=1)
            for half in range(2):
                bias[h, :, half * LANES:(half + 1) * LANES] = halves[half] + mask[...]

        crop = low if kind == "first" else mine
        base = me_p if kind == "first" else slot
        of = home_of if kind == "last" else cube_of

        def step(i, carry):
            w = lnw[p]
            zs_, ys, ks, qvs, os = [], [], [], [], []
            for q in range(ROWS):
                row = i * ROWS + q
                if kind == "first":
                    z = zin[row].astype(F32)
                else:
                    z = zf[pl.ds(row, n, stride=r), :]
                y = _ln(z, w)
                k = _dot(y, wk[p]).astype(BF16)
                qvt = _nt(wt[p], y)
                qq = qvt[:hd].astype(BF16)
                vv = qvt[hd:2 * hd].astype(BF16)
                t = qvt[2 * hd:] + jnp.concatenate([bg[p], bg[p]], axis=1)
                g = jax.nn.sigmoid(t)
                o = []
                for h in range(heads):
                    parts = [jnp.zeros((d, n), BF16)] * heads
                    parts[h] = qq[h * d:(h + 1) * d]
                    sc = _dot(k, jnp.concatenate(parts, axis=0)) * scale + bias[h]
                    e = jnp.exp2(sc - jnp.max(sc, axis=0, keepdims=True))
                    inv = 1.0 / jnp.sum(e, axis=0, keepdims=True)
                    oh = _dot(vv[h * d:(h + 1) * d], e.astype(BF16))
                    o.append((g[h * d:(h + 1) * d] * (oh * inv)).astype(BF16))
                upd = _tn(jnp.concatenate(o, axis=0), wo[p]) + bo[p]
                zn = (z + upd).astype(BF16)
                zout[row] = zn
                if kind != "last":
                    bout[row] = bias_rows(zn.astype(F32), lnw[p + 1], wb[p + 1])
            rows = pl.ds(i * ROWS, ROWS)
            dst = pl.ds(base * r + i * ROWS, ROWS)
            for s in range(nm):
                u = shifted(base, s)
                target = of(crop, u)
                send(zout.at[rows, pl.ds(pl.multiple_of(u * r, r), r)], zbuf.at[later, dst], zs, zr.at[later], target, kind, s)
                if kind != "last":
                    send(bout.at[rows], bbuf.at[later, dst], bs, br.at[later], target, kind, s)
            return carry
        lax.fori_loop(0, r // ROWS, step, 0)
        drain_sent(zout, zout.at[:, pl.ds(0, n - r)], zs, kind)
        if kind != "last":
            drain_sent(bbuf.at[now], bbuf.at[now, pl.ds(0, n - r)], bs, kind)

    run_pass(0, "first")

    def mid(p, carry):
        run_pass(p, "mid")
        return carry
    lax.fori_loop(1, last, mid, 0)
    run_pass(last, "last")

    end = 2
    drain(zbuf.at[end], zr.at[end])

    def widen(i, carry):
        rows = pl.ds(pl.multiple_of(i * r * r, r * r), r * r)
        zf[rows, :] = zbuf[end, pl.ds(i * r, r)].astype(F32).reshape(r * r, c)
        return carry
    lax.fori_loop(0, n // r, widen, 0)

    def finish(row, carry):
        out[row] = zf[pl.ds(row, n, stride=r), :].astype(BF16)
        return carry
    lax.fori_loop(0, r, finish, 0)


def solution(mesh):
    nd, nm = mesh.shape["data"], mesh.shape["dap"]

    def local(zl, res_mask, ln_w, w_in, b_g, w_b, w_o, b_o):
        r, n, c = zl.shape
        layers, two = w_in.shape[:2]
        m = layers * two
        hd, heads = w_o.shape[2], w_b.shape[3]
        w_in = w_in.reshape(m, c, 4, hd)
        wk = w_in[:, :, 1]
        wt = jnp.concatenate([w_in[:, :, 0], w_in[:, :, 2], w_in[:, :, 3]], axis=-1).swapaxes(1, 2)
        wbt = w_b.reshape(m, c, heads).swapaxes(1, 2)
        wb = jnp.concatenate([wbt, wbt], axis=1)
        bg = jnp.broadcast_to(b_g.astype(F32).reshape(m, hd, 1), (m, hd, LANES))
        maskb = jnp.broadcast_to(jnp.where(res_mask > 0, 0.0, NEG * LOG2E).astype(F32)[:, None], (n, LANES))
        vm = pl.BlockSpec(memory_space=pltpu.VMEM)
        return pl.pallas_call(
            functools.partial(_kernel, nd, nm),
            out_shape=jax.ShapeDtypeStruct((r, n, c), BF16),
            in_specs=[vm] * 9,
            out_specs=vm,
            scratch_shapes=[
                pltpu.VMEM((r, n, c), BF16),
                pltpu.VMEM((r, 2 * heads, LANES), BF16),
                pltpu.VMEM((3, n, r, c), BF16),
                pltpu.VMEM((3, n, 2 * heads, LANES), BF16),
                pltpu.VMEM((n * r, c), F32),
                pltpu.VMEM((n * 2 * heads, LANES), F32),
                pltpu.VMEM((heads, n, n), F32),
                pltpu.VMEM((2, n, LANES), F32),
                pltpu.SemaphoreType.DMA,
                pltpu.SemaphoreType.DMA,
                pltpu.SemaphoreType.DMA((3,)),
                pltpu.SemaphoreType.DMA((3,)),
                pltpu.SemaphoreType.DMA,
                pltpu.SemaphoreType.DMA,
            ],
            compiler_params=pltpu.CompilerParams(collective_id=0, has_side_effects=True, vmem_limit_bytes=56 * 1024 * 1024),
        )(zl, maskb, ln_w.astype(F32).reshape(m, 2, c), wk, wt, bg, wb,
          w_o.reshape(m, hd, c), b_o.astype(F32).reshape(m, 1, c))

    rows = P(('data', 'dap'))
    return jax.shard_map(local, mesh=mesh,
                         in_specs=(rows, P('data'), P(), P(), P(), P(), P(), P()),
                         out_specs=rows, check_vma=False)
```

```python
import functools
import math

import jax
import jax.numpy as jnp
from jax import lax
from jax.experimental import pallas as pl
from jax.experimental.pallas import tpu as pltpu
from jax.sharding import PartitionSpec as P

EPS = 1e-5
NEG = -1e9
LOG2E = math.log2(math.e)
F32 = jnp.float32
BF16 = jnp.bfloat16
MESH = pl.DeviceIdType.MESH
LANES = 128
LOOK = 3
ROWS = 4


def _ln(x, w):
    mu = jnp.mean(x, axis=-1, keepdims=True)
    xc = x - mu
    var = jnp.mean(xc * xc, axis=-1, keepdims=True)
    return (xc * lax.rsqrt(var + EPS) * w[0:1] + w[1:2]).astype(BF16)


def _nt(a, b):
    return lax.dot_general(a, b, (((1,), (1,)), ((), ())), preferred_element_type=F32)


def _tn(a, b):
    return lax.dot_general(a, b, (((0,), (0,)), ((), ())), preferred_element_type=F32)


def _dot(a, b):
    return jnp.dot(a, b, preferred_element_type=F32)


def _kernel(nd, nm, zin, maskb, lnw, wk, wt, bg, wb, wo, bo, out,
            zout, bout, zbuf, bbuf, zf, bf, bias, mbuf,
            zs, bs, zr, br, ms, mr):
    r, n, c = zin.shape
    passes, hd = wk.shape[0], wk.shape[2]
    heads = wb.shape[1] // 2
    d = hd // heads
    last = passes - 1
    scale = d ** -0.5 * LOG2E

    me_d, me_p = lax.axis_index("data"), lax.axis_index("dap")
    side = math.isqrt(nd)
    cube = side * side == nd and side % 2 == 0 and nm % 4 == 0
    if cube:
        sub = nm // 4
        x, y = me_d // side, me_d % side
        x0, y0 = x - x % 2, y - y % 2
        low = (x % 2) * 2 + y % 2
        mine = me_p // sub
        slot = low * sub + me_p % sub

        def home_of(crop, u):
            return (x0 + crop // 2) * side + y0 + crop % 2, u

        def cube_of(crop, u):
            lo = u // sub
            return (x0 + lo // 2) * side + y0 + lo % 2, crop * sub + u % sub
    else:
        low, mine, slot = me_d, me_d, me_p

        def home_of(crop, u):
            return me_d, u

        cube_of = home_of

    def is_me(t):
        return jnp.logical_and(t[0] == me_d, t[1] == me_p)

    def shifted(base, s):
        return (base + s) % nm

    inside = (low == mine) if cube else True

    def send(src, dst, ss, rs, target, kind, s):
        def local():
            pltpu.make_async_copy(src, dst, rs).start()

        def remote():
            pltpu.make_async_remote_copy(src, dst, ss, rs, device_id=target, device_id_type=MESH).start()

        if kind == "mid" or not cube:
            (local if s == 0 else remote)()
        else:
            me = is_me(target)
            pl.when(me)(local)
            pl.when(jnp.logical_not(me))(remote)

    def drain(ref, sem):
        pltpu.make_async_copy(ref, ref, sem).wait()

    def drain_sent(ref_all, ref_less, sem, kind):
        if kind == "mid" or not cube:
            drain(ref_less, sem)
        else:
            pl.when(inside)(lambda: drain(ref_less, sem))
            pl.when(jnp.logical_not(inside))(lambda: drain(ref_all, sem))

    barrier = pltpu.get_barrier_semaphore()
    groups = [(home_of, low), (cube_of, mine)] + ([(cube_of, low), (home_of, mine)] if cube else [])
    if not cube:
        groups = groups[:1]
    for of, crop in groups:
        def greet(u, carry, of=of, crop=crop):
            t = of(crop, u)

            @pl.when(jnp.logical_not(is_me(t)))
            def _():
                pl.semaphore_signal(barrier, inc=1, device_id=t, device_id_type=MESH)
            return carry
        lax.fori_loop(0, nm, greet, 0)
    if cube:
        @pl.when(inside)
        def _():
            pl.semaphore_wait(barrier, 4 * (nm - 1))

        @pl.when(jnp.logical_not(inside))
        def _():
            pl.semaphore_wait(barrier, 2 * (nm - 1) + 2 * nm)
    else:
        pl.semaphore_wait(barrier, nm - 1)

    low_half = lax.broadcasted_iota(jnp.int32, (2 * heads, LANES), 0) < heads

    def bias_rows(z, w, wbw):
        b = _nt(wbw, _ln(z, w))
        return jnp.where(low_half, b[:, :LANES], b[:, LANES:]).astype(BF16)

    mbuf[0] = maskb[...]
    mt = cube_of(low, me_p)
    if cube:
        me_m = is_me(mt)
        pl.when(me_m)(lambda: pltpu.make_async_copy(maskb, mbuf.at[1], mr).start())
        pl.when(jnp.logical_not(me_m))(lambda: pltpu.make_async_remote_copy(
            maskb, mbuf.at[1], ms, mr, device_id=mt, device_id_type=MESH).start())
    else:
        pltpu.make_async_copy(maskb, mbuf.at[1], mr).start()

    def first_bias(i, carry):
        w = lnw[0]
        for q in range(ROWS):
            row = i * ROWS + q
            bout[row] = bias_rows(zin[row].astype(F32), w, wb[0])
        return carry
    lax.fori_loop(0, r // ROWS, first_bias, 0)
    for s in range(nm):
        u = shifted(me_p, s)
        send(bout, bbuf.at[2, pl.ds(me_p * r, r)], bs, br.at[2], home_of(low, u), "mid", s)
    drain(bbuf.at[2], br.at[2])
    drain(bbuf.at[2, pl.ds(0, n - r)], bs)
    if cube:
        pl.when(jnp.logical_not(me_m))(lambda: drain(maskb, ms))
    drain(mbuf.at[1], mr)

    def run_pass(p, kind):
        now = 2 if kind == "first" else p % 2
        later = 2 if kind == "last" else (p + 1) % 2
        if kind != "first":
            drain(zbuf.at[now], zr.at[now])
            drain(bbuf.at[now], br.at[now])

            def widen(i, carry):
                rows = pl.ds(pl.multiple_of(i * r * r, r * r), r * r)
                zf[rows, :] = zbuf[now, pl.ds(i * r, r)].astype(F32).reshape(r * r, c)
                return carry
            lax.fori_loop(0, n // r, widen, 0)

        def widen_bias(i, carry):
            rows = pl.ds(pl.multiple_of(i * r * 2 * heads, r * 2 * heads), r * 2 * heads)
            bf[rows, :] = bbuf[now, pl.ds(i * r, r)].astype(F32).reshape(r * 2 * heads, LANES)
            return carry
        lax.fori_loop(0, n // r, widen_bias, 0)
        mask = mbuf.at[0 if kind == "first" else 1]
        for h in range(heads):
            halves = [bf[pl.ds(half * heads + h, n, stride=2 * heads), :] * LOG2E for half in range(2)]
            if kind == "first":
                halves = jnp.split(jnp.concatenate(halves, axis=1).T, 2, axis=1)
            for half in range(2):
                bias[h, :, half * LANES:(half + 1) * LANES] = halves[half] + mask[...]

        crop = low if kind == "first" else mine
        base = me_p if kind == "first" else slot
        of = home_of if kind == "last" else cube_of

        def step(i, carry):
            w = lnw[p]
            zrows, keys, queries, values, gates = [], [], [], [], []
            for q in range(ROWS):
                row = i * ROWS + q
                if kind == "first":
                    z = zin[row].astype(F32)
                else:
                    z = zf[pl.ds(row, n, stride=r), :]
                y = _ln(z, w)
                qvt = _nt(wt[p], y)
                zrows.append(z)
                keys.append(_dot(y, wk[p]).astype(BF16))
                queries.append(qvt[:hd].astype(BF16))
                values.append(qvt[hd:2 * hd].astype(BF16))
                gates.append(jax.nn.sigmoid(qvt[2 * hd:] + jnp.concatenate([bg[p], bg[p]], axis=1)))

            def scores(q, h):
                parts = [jnp.zeros((d, n), BF16)] * heads
                parts[h] = queries[q][h * d:(h + 1) * d]
                return _dot(keys[q], jnp.concatenate(parts, axis=0))

            units = [(q, h) for q in range(ROWS) for h in range(heads)]
            raw = [scores(*units[j]) for j in range(LOOK)]
            outs = []
            for j, (q, h) in enumerate(units):
                if j + LOOK < len(units):
                    raw.append(scores(*units[j + LOOK]))
                es, invs = [], []
                for cols in (slice(0, LANES), slice(LANES, 2 * LANES)):
                    sc = raw[j][:, cols] * scale + bias[h, :, cols]
                    e = jnp.exp2(sc - jnp.max(sc, axis=0, keepdims=True))
                    invs.append(1.0 / jnp.sum(e, axis=0, keepdims=True))
                    es.append(e.astype(BF16))
                span = slice(h * d, (h + 1) * d)
                oh = _dot(values[q][span], jnp.concatenate(es, axis=1)) * jnp.concatenate(invs, axis=1)
                outs.append((gates[q][span] * oh).astype(BF16))
            news = []
            for q in range(ROWS):
                upd = _tn(jnp.concatenate(outs[q * heads:(q + 1) * heads], axis=0), wo[p]) + bo[p]
                news.append((zrows[q] + upd).astype(BF16))
                zout[i * ROWS + q] = news[q]
            if kind != "last":
                for q in range(ROWS):
                    bout[i * ROWS + q] = bias_rows(news[q].astype(F32), lnw[p + 1], wb[p + 1])
            rows = pl.ds(i * ROWS, ROWS)
            dst = pl.ds(base * r + i * ROWS, ROWS)
            for s in range(nm):
                u = shifted(base, s)
                target = of(crop, u)
                send(zout.at[rows, pl.ds(pl.multiple_of(u * r, r), r)], zbuf.at[later, dst], zs, zr.at[later], target, kind, s)
                if kind != "last":
                    send(bout.at[rows], bbuf.at[later, dst], bs, br.at[later], target, kind, s)
            return carry
        lax.fori_loop(0, r // ROWS, step, 0)
        drain_sent(zout, zout.at[:, pl.ds(0, n - r)], zs, kind)
        if kind != "last":
            drain_sent(bbuf.at[now], bbuf.at[now, pl.ds(0, n - r)], bs, kind)

    run_pass(0, "first")

    def mid(p, carry):
        run_pass(p, "mid")
        return carry
    lax.fori_loop(1, last, mid, 0)
    run_pass(last, "last")

    end = 2
    drain(zbuf.at[end], zr.at[end])

    def widen(i, carry):
        rows = pl.ds(pl.multiple_of(i * r * r, r * r), r * r)
        zf[rows, :] = zbuf[end, pl.ds(i * r, r)].astype(F32).reshape(r * r, c)
        return carry
    lax.fori_loop(0, n // r, widen, 0)

    def finish(row, carry):
        out[row] = zf[pl.ds(row, n, stride=r), :].astype(BF16)
        return carry
    lax.fori_loop(0, r, finish, 0)


def solution(mesh):
    nd, nm = mesh.shape["data"], mesh.shape["dap"]

    def local(zl, res_mask, ln_w, w_in, b_g, w_b, w_o, b_o):
        r, n, c = zl.shape
        layers, two = w_in.shape[:2]
        m = layers * two
        hd, heads = w_o.shape[2], w_b.shape[3]
        w_in = w_in.reshape(m, c, 4, hd)
        wk = w_in[:, :, 1]
        wt = jnp.concatenate([w_in[:, :, 0], w_in[:, :, 2], w_in[:, :, 3]], axis=-1).swapaxes(1, 2)
        wbt = w_b.reshape(m, c, heads).swapaxes(1, 2)
        wb = jnp.concatenate([wbt, wbt], axis=1)
        bg = jnp.broadcast_to(b_g.astype(F32).reshape(m, hd, 1), (m, hd, LANES))
        maskb = jnp.broadcast_to(jnp.where(res_mask > 0, 0.0, NEG * LOG2E).astype(F32)[:, None], (n, LANES))
        vm = pl.BlockSpec(memory_space=pltpu.VMEM)
        return pl.pallas_call(
            functools.partial(_kernel, nd, nm),
            out_shape=jax.ShapeDtypeStruct((r, n, c), BF16),
            in_specs=[vm] * 9,
            out_specs=vm,
            scratch_shapes=[
                pltpu.VMEM((r, n, c), BF16),
                pltpu.VMEM((r, 2 * heads, LANES), BF16),
                pltpu.VMEM((3, n, r, c), BF16),
                pltpu.VMEM((3, n, 2 * heads, LANES), BF16),
                pltpu.VMEM((n * r, c), F32),
                pltpu.VMEM((n * 2 * heads, LANES), F32),
                pltpu.VMEM((heads, n, n), F32),
                pltpu.VMEM((2, n, LANES), F32),
                pltpu.SemaphoreType.DMA,
                pltpu.SemaphoreType.DMA,
                pltpu.SemaphoreType.DMA((3,)),
                pltpu.SemaphoreType.DMA((3,)),
                pltpu.SemaphoreType.DMA,
                pltpu.SemaphoreType.DMA,
            ],
            compiler_params=pltpu.CompilerParams(collective_id=0, has_side_effects=True, vmem_limit_bytes=56 * 1024 * 1024),
        )(zl, maskb, ln_w.astype(F32).reshape(m, 2, c), wk, wt, bg, wb,
          w_o.reshape(m, hd, c), b_o.astype(F32).reshape(m, 1, c))

    rows = P(('data', 'dap'))
    return jax.shard_map(local, mesh=mesh,
                         in_specs=(rows, P('data'), P(), P(), P(), P(), P(), P()),
                         out_specs=rows, check_vma=False)
```

```python
import functools
import math

import jax
import jax.numpy as jnp
from jax import lax
from jax.experimental import pallas as pl
from jax.experimental.pallas import tpu as pltpu
from jax.sharding import PartitionSpec as P

EPS = 1e-5
NEG = -1e9
LOG2E = math.log2(math.e)
F32 = jnp.float32
BF16 = jnp.bfloat16
MESH = pl.DeviceIdType.MESH
LANES = 128
LOOK = 3
AHEAD = 2
ROWS = 8
CHUNK = 2
EDGE_ROWS = 4


def _ln(x, w):
    mu = jnp.mean(x, axis=-1, keepdims=True)
    xc = x - mu
    var = jnp.mean(xc * xc, axis=-1, keepdims=True)
    return (xc * lax.rsqrt(var + EPS) * w[0:1] + w[1:2]).astype(BF16)


def _nt(a, b):
    return lax.dot_general(a, b, (((1,), (1,)), ((), ())), preferred_element_type=F32)


def _tn(a, b):
    return lax.dot_general(a, b, (((0,), (0,)), ((), ())), preferred_element_type=F32)


def _dot(a, b):
    return jnp.dot(a, b, preferred_element_type=F32)


def _kernel(nd, nm, zin, maskb, lnw, wk, wt, bg, wb, wo, bo, out,
            zout, bout, zbuf, bbuf, zf, bf, bias, mbuf,
            zs, bs, fs, zr, br, fr, ms, mr):
    r, n, c = zin.shape
    passes, hd = wk.shape[0], wk.shape[2]
    heads = wb.shape[1] // 2
    d = hd // heads
    last = passes - 1
    scale = d ** -0.5 * LOG2E

    me_d, me_p = lax.axis_index("data"), lax.axis_index("dap")
    side = math.isqrt(nd)
    cube = side * side == nd and side % 2 == 0 and nm % 4 == 0
    if cube:
        sub = nm // 4
        x, y = me_d // side, me_d % side
        x0, y0 = x - x % 2, y - y % 2
        low = (x % 2) * 2 + y % 2
        mine = me_p // sub
        slot = low * sub + me_p % sub

        def home_of(crop, u):
            return (x0 + crop // 2) * side + y0 + crop % 2, u

        def cube_of(crop, u):
            lo = u // sub
            return (x0 + lo // 2) * side + y0 + lo % 2, crop * sub + u % sub
    else:
        low, mine, slot = me_d, me_d, me_p

        def home_of(crop, u):
            return me_d, u

        cube_of = home_of

    def is_me(t):
        return jnp.logical_and(t[0] == me_d, t[1] == me_p)

    def shifted(base, s):
        return (base + s) % nm

    inside = (low == mine) if cube else True

    def send(src, dst, ss, rs, target, kind, s):
        def local():
            pltpu.make_async_copy(src, dst, rs).start()

        def remote():
            pltpu.make_async_remote_copy(src, dst, ss, rs, device_id=target, device_id_type=MESH).start()

        if kind == "mid" or not cube:
            (local if s == 0 else remote)()
        else:
            me = is_me(target)
            pl.when(me)(local)
            pl.when(jnp.logical_not(me))(remote)

    def drain(ref, sem):
        pltpu.make_async_copy(ref, ref, sem).wait()

    def drain_sent(ref_all, ref_less, sem, kind):
        if kind == "mid" or not cube:
            drain(ref_less, sem)
        else:
            pl.when(inside)(lambda: drain(ref_less, sem))
            pl.when(jnp.logical_not(inside))(lambda: drain(ref_all, sem))

    core = me_p % 2

    def hand_on(slot_):
        half = bbuf.at[slot_, :, core]
        drain(half, br.at[slot_])
        pltpu.make_async_remote_copy(half, half, fs, fr.at[slot_], device_id=(me_d, me_p + 1 - 2 * core),
                                     device_id_type=MESH).start()

    def handed_on(slot_):
        half = bbuf.at[slot_, :, core]
        drain(half, fr.at[slot_])
        drain(half, fs)

    barrier = pltpu.get_barrier_semaphore()
    groups = [(home_of, low), (cube_of, mine)] + ([(cube_of, low), (home_of, mine)] if cube else [])
    if not cube:
        groups = groups[:1]
    for of, crop in groups:
        def greet(u, carry, of=of, crop=crop):
            t = of(crop, u)

            @pl.when(jnp.logical_not(is_me(t)))
            def _():
                pl.semaphore_signal(barrier, inc=1, device_id=t, device_id_type=MESH)
            return carry
        lax.fori_loop(0, nm, greet, 0)
    if cube:
        @pl.when(inside)
        def _():
            pl.semaphore_wait(barrier, 4 * (nm - 1))

        @pl.when(jnp.logical_not(inside))
        def _():
            pl.semaphore_wait(barrier, 2 * (nm - 1) + 2 * nm)
    else:
        pl.semaphore_wait(barrier, nm - 1)

    low_half = lax.broadcasted_iota(jnp.int32, (2 * heads, LANES), 0) < heads

    def bias_rows(z, w, wbw):
        b = _nt(wbw, _ln(z, w))
        return jnp.where(low_half, b[:, :LANES], b[:, LANES:]).astype(BF16)

    mbuf[0] = maskb[...]
    mt = cube_of(low, me_p)
    if cube:
        me_m = is_me(mt)
        pl.when(me_m)(lambda: pltpu.make_async_copy(maskb, mbuf.at[1], mr).start())
        pl.when(jnp.logical_not(me_m))(lambda: pltpu.make_async_remote_copy(
            maskb, mbuf.at[1], ms, mr, device_id=mt, device_id_type=MESH).start())
    else:
        pltpu.make_async_copy(maskb, mbuf.at[1], mr).start()

    def first_bias(i, carry):
        w = lnw[0]
        for q in range(EDGE_ROWS):
            row = i * EDGE_ROWS + q
            bout[row] = bias_rows(zin[row].astype(F32), w, wb[0])
        return carry
    lax.fori_loop(0, r // EDGE_ROWS, first_bias, 0)
    for s in range(0, nm, 2):
        u = shifted(me_p, s)
        send(bout, bbuf.at[2, me_p // 2, core], bs, br.at[2], home_of(low, u), "mid", s)
    hand_on(2)
    drain(bbuf.at[2, pl.ds(0, nm // 2 - 1), core], bs)
    handed_on(2)
    if cube:
        pl.when(jnp.logical_not(me_m))(lambda: drain(maskb, ms))
    drain(mbuf.at[1], mr)

    def run_pass(p, kind):
        now = 2 if kind == "first" else p % 2
        later = 2 if kind == "last" else (p + 1) % 2
        if kind != "first":
            hand_on(now)
            drain(zbuf.at[now], zr.at[now])

            def widen(i, carry):
                rows = pl.ds(pl.multiple_of(i * r * r, r * r), r * r)
                zf[rows, :] = zbuf[now, pl.ds(i * r, r)].astype(F32).reshape(r * r, c)
                return carry
            lax.fori_loop(0, n // r, widen, 0)
            handed_on(now)

        def widen_bias(i, carry):
            rows = pl.ds(pl.multiple_of(i * r * 2 * heads, r * 2 * heads), r * 2 * heads)
            bf[rows, :] = bbuf[now, i // 2, i % 2].astype(F32).reshape(r * 2 * heads, LANES)
            return carry
        lax.fori_loop(0, n // r, widen_bias, 0)
        mask = mbuf.at[0 if kind == "first" else 1]
        for h in range(heads):
            halves = [bf[pl.ds(half * heads + h, n, stride=2 * heads), :] * LOG2E for half in range(2)]
            if kind == "first":
                halves = jnp.split(jnp.concatenate(halves, axis=1).T, 2, axis=1)
            for half in range(2):
                bias[h, :, half * LANES:(half + 1) * LANES] = halves[half] + mask[...]

        crop = low if kind == "first" else mine
        base = me_p if kind == "first" else slot
        of = home_of if kind == "last" else cube_of

        def post(first_row, count):
            rows = pl.ds(first_row, count)
            for s in range(nm):
                u = shifted(base, s)
                target = of(crop, u)
                if kind != "last" and s % 2 == 0:
                    send(bout.at[rows], bbuf.at[later, base // 2, core, rows], bs, br.at[later], target, kind, s)
                send(zout.at[rows, pl.ds(pl.multiple_of(u * r, r), r)],
                     zbuf.at[later, pl.ds(base * r + first_row, count)], zs, zr.at[later], target, kind, s)

        def attend(first_row, count, chunk):
            w = lnw[p]
            gate_b = jnp.concatenate([bg[p], bg[p]], axis=1)
            zrows, keys, queries, values, gates, raw, outs, news = [], [], [], [], [], [], [], []
            units = [(q, h) for q in range(count) for h in range(heads)]

            def project(q):
                row = first_row + q
                z = zin[row].astype(F32) if kind == "first" else zf[pl.ds(row, n, stride=r), :]
                y = _ln(z, w)
                qvt = _nt(wt[p], y)
                zrows.append(z)
                keys.append(_dot(y, wk[p]).astype(BF16))
                queries.append(qvt[:hd].astype(BF16))
                values.append(qvt[hd:2 * hd].astype(BF16))
                gates.append(jax.nn.sigmoid(qvt[2 * hd:] + gate_b))

            def scores(q, h):
                parts = [jnp.zeros((d, n), BF16)] * heads
                parts[h] = queries[q][h * d:(h + 1) * d]
                return _dot(keys[q], jnp.concatenate(parts, axis=0))

            def update(q):
                upd = _tn(jnp.concatenate(outs[q * heads:(q + 1) * heads], axis=0), wo[p]) + bo[p]
                news.append((zrows[q] + upd).astype(BF16))
                zout[first_row + q] = news[q]

            def finish_row(q):
                if kind != "last":
                    bout[first_row + q] = bias_rows(news[q].astype(F32), lnw[p + 1], wb[p + 1])
                if (q + 1) % chunk == 0:
                    post(first_row + q + 1 - chunk, chunk)

            for q in range(min(AHEAD, count)):
                project(q)
            for j in range(LOOK):
                raw.append(scores(*units[j]))
            for j, (q, h) in enumerate(units):
                if h == 0 and q + AHEAD < count:
                    project(q + AHEAD)
                if j + LOOK < len(units):
                    raw.append(scores(*units[j + LOOK]))
                es, invs = [], []
                for cols in (slice(0, LANES), slice(LANES, 2 * LANES)):
                    sc = raw[j][:, cols] * scale + bias[h, :, cols]
                    e = jnp.exp2(sc - jnp.max(sc, axis=0, keepdims=True))
                    invs.append(1.0 / jnp.sum(e, axis=0, keepdims=True))
                    es.append(e.astype(BF16))
                span = slice(h * d, (h + 1) * d)
                oh = _dot(values[q][span], jnp.concatenate(es, axis=1)) * jnp.concatenate(invs, axis=1)
                outs.append((gates[q][span] * oh).astype(BF16))
                if h == 1 and q > 0:
                    update(q - 1)
                if h == 3 and q > 0:
                    finish_row(q - 1)
            update(count - 1)
            finish_row(count - 1)

        block, chunk = (ROWS, CHUNK) if kind == "mid" else (EDGE_ROWS, EDGE_ROWS)

        def step(i, carry):
            attend(i * block, block, chunk)
            return carry
        lax.fori_loop(0, r // block, step, 0)
        drain_sent(zout, zout.at[:, pl.ds(0, n - r)], zs, kind)
        if kind != "last":
            drain_sent(bbuf.at[now, :, core], bbuf.at[now, pl.ds(0, nm // 2 - 1), core], bs, kind)

    run_pass(0, "first")

    def mid(p, carry):
        run_pass(p, "mid")
        return carry
    lax.fori_loop(1, last, mid, 0)
    run_pass(last, "last")

    end = 2
    drain(zbuf.at[end], zr.at[end])

    def widen(i, carry):
        rows = pl.ds(pl.multiple_of(i * r * r, r * r), r * r)
        zf[rows, :] = zbuf[end, pl.ds(i * r, r)].astype(F32).reshape(r * r, c)
        return carry
    lax.fori_loop(0, n // r, widen, 0)

    def finish(row, carry):
        out[row] = zf[pl.ds(row, n, stride=r), :].astype(BF16)
        return carry
    lax.fori_loop(0, r, finish, 0)


def solution(mesh):
    nd, nm = mesh.shape["data"], mesh.shape["dap"]

    def local(zl, res_mask, ln_w, w_in, b_g, w_b, w_o, b_o):
        r, n, c = zl.shape
        layers, two = w_in.shape[:2]
        m = layers * two
        hd, heads = w_o.shape[2], w_b.shape[3]
        w_in = w_in.reshape(m, c, 4, hd)
        wk = w_in[:, :, 1]
        wt = jnp.concatenate([w_in[:, :, 0], w_in[:, :, 2], w_in[:, :, 3]], axis=-1).swapaxes(1, 2)
        wbt = w_b.reshape(m, c, heads).swapaxes(1, 2)
        wb = jnp.concatenate([wbt, wbt], axis=1)
        bg = jnp.broadcast_to(b_g.astype(F32).reshape(m, hd, 1), (m, hd, LANES))
        maskb = jnp.broadcast_to(jnp.where(res_mask > 0, 0.0, NEG * LOG2E).astype(F32)[:, None], (n, LANES))
        vm = pl.BlockSpec(memory_space=pltpu.VMEM)
        return pl.pallas_call(
            functools.partial(_kernel, nd, nm),
            out_shape=jax.ShapeDtypeStruct((r, n, c), BF16),
            in_specs=[vm] * 9,
            out_specs=vm,
            scratch_shapes=[
                pltpu.VMEM((r, n, c), BF16),
                pltpu.VMEM((r, 2 * heads, LANES), BF16),
                pltpu.VMEM((3, n, r, c), BF16),
                pltpu.VMEM((3, nm // 2, 2, r, 2 * heads, LANES), BF16),
                pltpu.VMEM((n * r, c), F32),
                pltpu.VMEM((n * 2 * heads, LANES), F32),
                pltpu.VMEM((heads, n, n), F32),
                pltpu.VMEM((2, n, LANES), F32),
                pltpu.SemaphoreType.DMA,
                pltpu.SemaphoreType.DMA,
                pltpu.SemaphoreType.DMA,
                pltpu.SemaphoreType.DMA((3,)),
                pltpu.SemaphoreType.DMA((3,)),
                pltpu.SemaphoreType.DMA((3,)),
                pltpu.SemaphoreType.DMA,
                pltpu.SemaphoreType.DMA,
            ],
            compiler_params=pltpu.CompilerParams(collective_id=0, has_side_effects=True, vmem_limit_bytes=56 * 1024 * 1024),
        )(zl, maskb, ln_w.astype(F32).reshape(m, 2, c), wk, wt, bg, wb,
          w_o.reshape(m, hd, c), b_o.astype(F32).reshape(m, 1, c))

    rows = P(('data', 'dap'))
    return jax.shard_map(local, mesh=mesh,
                         in_specs=(rows, P('data'), P(), P(), P(), P(), P(), P()),
                         out_specs=rows, check_vma=False)
```

```python
import functools
import math

import jax
import jax.numpy as jnp
from jax import lax
from jax.experimental import pallas as pl
from jax.experimental.pallas import tpu as pltpu
from jax.sharding import PartitionSpec as P

EPS = 1e-5
NEG = -1e9
LOG2E = math.log2(math.e)
F32 = jnp.float32
BF16 = jnp.bfloat16
MESH = pl.DeviceIdType.MESH
LANES = 128
LOOK = 3
AHEAD = 2
ROWS = 8
CHUNK = 2
EDGE_ROWS = 4


def _ln(x, w):
    mu = jnp.mean(x, axis=-1, keepdims=True)
    xc = x - mu
    var = jnp.mean(xc * xc, axis=-1, keepdims=True)
    return (xc * lax.rsqrt(var + EPS) * w[0:1] + w[1:2]).astype(BF16)


def _nt(a, b):
    return lax.dot_general(a, b, (((1,), (1,)), ((), ())), preferred_element_type=F32)


def _tn(a, b):
    return lax.dot_general(a, b, (((0,), (0,)), ((), ())), preferred_element_type=F32)


def _dot(a, b):
    return jnp.dot(a, b, preferred_element_type=F32)


def _kernel(nd, nm, zin, maskb, small, win, wb, wo, out,
            zout, bout, zbuf, bbuf, zf, bf, bias, mbuf, wt, zrelay, brelay,
            zs, bs, fs, zr, br, fr, ms, mr, rs, zrr, brr):
    r, n, c = zin.shape
    passes, hd = wo.shape[0], wo.shape[1]
    heads = wb.shape[1] // 2
    d = hd // heads
    last = passes - 1
    scale = d ** -0.5 * LOG2E

    me_d, me_p = lax.axis_index("data"), lax.axis_index("dap")
    side = math.isqrt(nd)
    cube = side * side == nd and side % 2 == 0 and nm % 4 == 0
    if cube:
        sub = nm // 4
        x, y = me_d // side, me_d % side
        x0, y0 = x - x % 2, y - y % 2
        low = (x % 2) * 2 + y % 2
        mine = me_p // sub
        slot = low * sub + me_p % sub

        def home_of(crop, u):
            return (x0 + crop // 2) * side + y0 + crop % 2, u

        def cube_of(crop, u):
            lo = u // sub
            return (x0 + lo // 2) * side + y0 + lo % 2, crop * sub + u % sub
    else:
        low, mine, slot = me_d, me_d, me_p

        def home_of(crop, u):
            return me_d, u

        cube_of = home_of

    hslot = me_p

    def is_me(t):
        return jnp.logical_and(t[0] == me_d, t[1] == me_p)

    def shifted(base, s):
        return (base + s) % nm

    inside = (low == mine) if cube else True

    def send(src, dst, ss, rs, target, kind, s):
        def local():
            pltpu.make_async_copy(src, dst, rs).start()

        def remote():
            pltpu.make_async_remote_copy(src, dst, ss, rs, device_id=target, device_id_type=MESH).start()

        if kind == "mid" or not cube:
            (local if s == 0 else remote)()
        else:
            me = is_me(target)
            pl.when(me)(local)
            pl.when(jnp.logical_not(me))(remote)

    def drain(ref, sem):
        pltpu.make_async_copy(ref, ref, sem).wait()

    def drain_sent(ref_all, ref_less, sem, kind):
        if kind != "last" or not cube:
            drain(ref_less, sem)
        else:
            pl.when(inside)(lambda: drain(ref_less, sem))
            pl.when(jnp.logical_not(inside))(lambda: drain(ref_all, sem))

    core = me_p % 2

    def hand_on(slot_):
        half = bbuf.at[slot_, :, core]
        drain(half, br.at[slot_])
        pltpu.make_async_remote_copy(half, half, fs, fr.at[slot_], device_id=(me_d, me_p + 1 - 2 * core),
                                     device_id_type=MESH).start()

    def handed_on(slot_):
        half = bbuf.at[slot_, :, core]
        drain(half, fr.at[slot_])
        drain(half, fs)

    barrier = pltpu.get_barrier_semaphore()
    groups = [(home_of, low), (cube_of, mine)] + ([(cube_of, low), (home_of, mine)] if cube else [])
    if not cube:
        groups = groups[:1]
    for of, crop in groups:
        def greet(u, carry, of=of, crop=crop):
            t = of(crop, u)

            @pl.when(jnp.logical_not(is_me(t)))
            def _():
                pl.semaphore_signal(barrier, inc=1, device_id=t, device_id_type=MESH)
            return carry
        lax.fori_loop(0, nm, greet, 0)
    if cube:
        for s in range(1, 4):
            pl.semaphore_signal(barrier, inc=1, device_id=home_of((low + s) % 4, me_p), device_id_type=MESH)

        @pl.when(inside)
        def _():
            pl.semaphore_wait(barrier, 4 * (nm - 1) + 3)

        @pl.when(jnp.logical_not(inside))
        def _():
            pl.semaphore_wait(barrier, 2 * (nm - 1) + 2 * nm + 3)
    else:
        pl.semaphore_wait(barrier, nm - 1)

    low_half = lax.broadcasted_iota(jnp.int32, (2 * heads, LANES), 0) < heads

    def bias_rows(z, w, wbw):
        b = _nt(wbw, _ln(z, w))
        return jnp.where(low_half, b[:, :LANES], b[:, LANES:]).astype(BF16)

    mt = cube_of(low, hslot)
    if cube:
        me_m = is_me(mt)
        pl.when(me_m)(lambda: pltpu.make_async_copy(maskb, mbuf, mr).start())
        pl.when(jnp.logical_not(me_m))(lambda: pltpu.make_async_remote_copy(
            maskb, mbuf, ms, mr, device_id=mt, device_id_type=MESH).start())
    else:
        pltpu.make_async_copy(maskb, mbuf, mr).start()

    def first_bias(i, carry):
        w = small[0]
        for q in range(EDGE_ROWS):
            row = i * EDGE_ROWS + q
            bout[row] = bias_rows(zin[row].astype(F32), w, wb[0])
        return carry
    lax.fori_loop(0, r // EDGE_ROWS, first_bias, 0)
    for s in range(0, nm, 2):
        u = shifted(hslot, s)
        send(bout, bbuf.at[2, hslot // 2, core], bs, br.at[2], home_of(low, u), "mid", s)

    def turn(i, carry):
        for t, part in enumerate((0, 2, 3)):
            wt[i, t * hd:(t + 1) * hd] = win[i, :, part * hd:(part + 1) * hd].T
        return carry
    lax.fori_loop(0, passes, turn, 0)
    hand_on(2)
    drain(bbuf.at[2, pl.ds(0, nm // 2 - 1), core], bs)
    handed_on(2)
    if cube:
        pl.when(jnp.logical_not(me_m))(lambda: drain(maskb, ms))
    drain(mbuf, mr)

    def run_pass(p, kind):
        now = 2 if kind == "first" else p % 2
        later = 2 if kind == "last" else (p + 1) % 2
        if kind != "first":
            hand_on(now)
            drain(zbuf.at[now], zr.at[now])

            def widen(i, carry):
                rows = pl.ds(pl.multiple_of(i * r * r, r * r), r * r)
                zf[rows, :] = zbuf[now, pl.ds(i * r, r)].astype(F32).reshape(r * r, c)
                return carry
            lax.fori_loop(0, n // r, widen, 0)
            handed_on(now)

        def widen_bias(i, carry):
            rows = pl.ds(pl.multiple_of(i * r * 2 * heads, r * 2 * heads), r * 2 * heads)
            bf[rows, :] = bbuf[now, i // 2, i % 2].astype(F32).reshape(r * 2 * heads, LANES)
            return carry
        lax.fori_loop(0, n // r, widen_bias, 0)
        mask_row = (maskb if kind == "first" else mbuf)[...]
        mask = jnp.concatenate([jnp.broadcast_to(mask_row[t:t + 1], (LANES, LANES)).T for t in range(n // LANES)], axis=0)
        for h in range(heads):
            halves = [bf[pl.ds(half * heads + h, n, stride=2 * heads), :] * LOG2E for half in range(2)]
            if kind == "first":
                halves = jnp.split(jnp.concatenate(halves, axis=1).T, 2, axis=1)
            for half in range(2):
                bias[h, :, half * LANES:(half + 1) * LANES] = halves[half] + mask

        crop = low if kind == "first" else mine
        base = hslot if kind == "first" else slot
        of = home_of if kind == "last" else cube_of

        def post(first_row, count):
            rows = pl.ds(first_row, count)
            for s in range(nm):
                u = shifted(base, s)
                target = of(crop, u)
                if kind != "last" and s % 2 == 0:
                    send(bout.at[rows], bbuf.at[later, base // 2, core, rows], bs, br.at[later], target, kind, s)
                send(zout.at[rows, pl.ds(pl.multiple_of(u * r, r), r)],
                     zbuf.at[later, pl.ds(base * r + first_row, count)], zs, zr.at[later], target, kind, s)

        def spread(i, count):
            rows = pl.ds(i * count, count)
            for s in range(4):
                lo = (low + s) % 4
                cols = pl.ds(pl.multiple_of(lo * sub * r, r), sub * r)
                target = home_of(lo, me_p)
                send(bout.at[rows], brelay.at[low, rows], rs.at[0], brr.at[i], target, "mid", s)
                send(zout.at[rows, cols], zrelay.at[low, rows], rs.at[1], zrr.at[i], target, "mid", s)

        def relay(i, count):
            rows = pl.ds(i * count, count)
            drain(brelay.at[:, rows], brr.at[i])
            drain(zrelay.at[:, rows], zrr.at[i])
            for s in range(nm):
                u = shifted(me_p, s)
                to = u // sub
                if s % 2 == 0:
                    send(brelay.at[to, rows], bbuf.at[later, me_p // 2, core, rows], bs, br.at[later], (me_d, u), "mid", s)
                cols = pl.ds(pl.multiple_of((u % sub) * r, r), r)
                send(zrelay.at[to, rows, cols], zbuf.at[later, pl.ds(me_p * r + i * count, count)],
                     zs, zr.at[later], (me_d, u), "mid", s)

        def attend(first_row, count, chunk):
            par = small[p]
            w = par[0:2]
            out_b = par[3:4]
            gate_b = jnp.broadcast_to(par[2:3], (n, hd)).T
            zrows, keys, queries, values, gates, raw, outs, news = [], [], [], [], [], [], [], []
            units = [(q, h) for q in range(count) for h in range(heads)]

            def project(q):
                row = first_row + q
                z = zin[row].astype(F32) if kind == "first" else zf[pl.ds(row, n, stride=r), :]
                y = _ln(z, w)
                qvt = _nt(wt[p], y)
                zrows.append(z)
                keys.append(_dot(y, win[p, :, hd:2 * hd]).astype(BF16))
                queries.append(qvt[:hd].astype(BF16))
                values.append(qvt[hd:2 * hd].astype(BF16))
                gates.append(jax.nn.sigmoid(qvt[2 * hd:] + gate_b))

            def scores(q, h):
                parts = [jnp.zeros((d, n), BF16)] * heads
                parts[h] = queries[q][h * d:(h + 1) * d]
                return _dot(keys[q], jnp.concatenate(parts, axis=0))

            def update(q):
                upd = _tn(jnp.concatenate(outs[q * heads:(q + 1) * heads], axis=0), wo[p]) + out_b
                news.append((zrows[q] + upd).astype(BF16))
                zout[first_row + q] = news[q]

            def finish_row(q):
                if kind != "last":
                    bout[first_row + q] = bias_rows(news[q].astype(F32), small[p + 1], wb[p + 1])
                if (q + 1) % chunk == 0 and not (cube and kind == "first"):
                    post(first_row + q + 1 - chunk, chunk)

            for q in range(min(AHEAD, count)):
                project(q)
            for j in range(LOOK):
                raw.append(scores(*units[j]))
            for j, (q, h) in enumerate(units):
                if h == 0 and q + AHEAD < count:
                    project(q + AHEAD)
                if j + LOOK < len(units):
                    raw.append(scores(*units[j + LOOK]))
                es, invs = [], []
                for cols in (slice(0, LANES), slice(LANES, 2 * LANES)):
                    sc = raw[j][:, cols] * scale + bias[h, :, cols]
                    e = jnp.exp2(sc - jnp.max(sc, axis=0, keepdims=True))
                    invs.append(1.0 / jnp.sum(e, axis=0, keepdims=True))
                    es.append(e.astype(BF16))
                span = slice(h * d, (h + 1) * d)
                oh = _dot(values[q][span], jnp.concatenate(es, axis=1)) * jnp.concatenate(invs, axis=1)
                outs.append((gates[q][span] * oh).astype(BF16))
                if h == 1 and q > 0:
                    update(q - 1)
                if h == 3 and q > 0:
                    finish_row(q - 1)
            update(count - 1)
            finish_row(count - 1)

        block, chunk = (ROWS, CHUNK) if kind == "mid" else (EDGE_ROWS, EDGE_ROWS)

        def step(i, carry):
            attend(i * block, block, chunk)
            if cube and kind == "first":
                spread(i, block)
                pl.when(i > 0)(lambda: relay(i - 1, block))
            return carry
        lax.fori_loop(0, r // block, step, 0)
        if cube and kind == "first":
            relay(r // block - 1, block)
            drain(zrelay.at[pl.ds(0, 3)], rs.at[1])
            drain(brelay.at[pl.ds(0, 3)], rs.at[0])
        drain_sent(zout, zout.at[:, pl.ds(0, n - r)], zs, kind)
        if kind != "last":
            drain_sent(bbuf.at[now, :, core], bbuf.at[now, pl.ds(0, nm // 2 - 1), core], bs, kind)

    run_pass(0, "first")

    def mid(p, carry):
        run_pass(p, "mid")
        return carry
    lax.fori_loop(1, last, mid, 0)
    run_pass(last, "last")

    end = 2
    drain(zbuf.at[end], zr.at[end])

    def widen(i, carry):
        rows = pl.ds(pl.multiple_of(i * r * r, r * r), r * r)
        zf[rows, :] = zbuf[end, pl.ds(i * r, r)].astype(F32).reshape(r * r, c)
        return carry
    lax.fori_loop(0, n // r, widen, 0)

    def finish(row, carry):
        out[row] = zf[pl.ds(row, n, stride=r), :].astype(BF16)
        return carry
    lax.fori_loop(0, r, finish, 0)


def solution(mesh):
    nd, nm = mesh.shape["data"], mesh.shape["dap"]

    def local(zl, res_mask, ln_w, w_in, b_g, w_b, w_o, b_o):
        r, n, c = zl.shape
        layers, two = w_in.shape[:2]
        m = layers * two
        hd, heads = w_o.shape[2], w_b.shape[3]
        wbt = w_b.reshape(m, c, heads).swapaxes(1, 2)
        wb = jnp.concatenate([wbt, wbt], axis=1)
        small = jnp.concatenate([ln_w, b_g[:, :, None], b_o[:, :, None]], axis=2).astype(F32).reshape(m, 4, c)
        maskb = jnp.where(res_mask > 0, 0.0, NEG * LOG2E).astype(F32).reshape(n // LANES, LANES)
        maskb = jnp.pad(maskb, ((0, 8 - n // LANES), (0, 0)))
        vm = pl.BlockSpec(memory_space=pltpu.VMEM)
        return pl.pallas_call(
            functools.partial(_kernel, nd, nm),
            out_shape=jax.ShapeDtypeStruct((r, n, c), BF16),
            in_specs=[vm] * 6,
            out_specs=vm,
            scratch_shapes=[
                pltpu.VMEM((r, n, c), BF16),
                pltpu.VMEM((r, 2 * heads, LANES), BF16),
                pltpu.VMEM((3, n, r, c), BF16),
                pltpu.VMEM((3, nm // 2, 2, r, 2 * heads, LANES), BF16),
                pltpu.VMEM((n * r, c), F32),
                pltpu.VMEM((n * 2 * heads, LANES), F32),
                pltpu.VMEM((heads, n, n), F32),
                pltpu.VMEM((8, LANES), F32),
                pltpu.VMEM((m, 3 * hd, c), BF16),
                pltpu.VMEM((4, r, n // 4, c), BF16),
                pltpu.VMEM((4, r, 2 * heads, LANES), BF16),
                pltpu.SemaphoreType.DMA,
                pltpu.SemaphoreType.DMA,
                pltpu.SemaphoreType.DMA,
                pltpu.SemaphoreType.DMA((3,)),
                pltpu.SemaphoreType.DMA((3,)),
                pltpu.SemaphoreType.DMA((3,)),
                pltpu.SemaphoreType.DMA,
                pltpu.SemaphoreType.DMA,
                pltpu.SemaphoreType.DMA((2,)),
                pltpu.SemaphoreType.DMA((r // EDGE_ROWS,)),
                pltpu.SemaphoreType.DMA((r // EDGE_ROWS,)),
            ],
            compiler_params=pltpu.CompilerParams(collective_id=0, has_side_effects=True, vmem_limit_bytes=56 * 1024 * 1024),
        )(zl, maskb, small, w_in.reshape(m, c, 4 * hd), wb, w_o.reshape(m, hd, c))

    rows = P(('data', 'dap'))
    return jax.shard_map(local, mesh=mesh,
                         in_specs=(rows, P('data'), P(), P(), P(), P(), P(), P()),
                         out_specs=rows, check_vma=False)
```

```python
import functools
import math

import jax
import jax.numpy as jnp
from jax import lax
from jax.experimental import pallas as pl
from jax.experimental.pallas import tpu as pltpu
from jax.sharding import PartitionSpec as P

EPS = 1e-5
NEG = -1e9
LOG2E = math.log2(math.e)
F32 = jnp.float32
BF16 = jnp.bfloat16
MESH = pl.DeviceIdType.MESH
LANES = 128
LOOK = 3
AHEAD = 2
ROWS = 4
CHUNKS = (2, 4)
BIAS_ROWS = 4
EDGE_ROWS = 4


def _ln(x, w):
    mu = jnp.mean(x, axis=-1, keepdims=True)
    xc = x - mu
    var = jnp.mean(xc * xc, axis=-1, keepdims=True)
    return (xc * lax.rsqrt(var + EPS) * w[0:1] + w[1:2]).astype(BF16)


def _nt(a, b):
    return lax.dot_general(a, b, (((1,), (1,)), ((), ())), preferred_element_type=F32)


def _tn(a, b):
    return lax.dot_general(a, b, (((0,), (0,)), ((), ())), preferred_element_type=F32)


def _dot(a, b):
    return jnp.dot(a, b, preferred_element_type=F32)


def _kernel(nd, nm, zin, maskb, small, win, wb, wo, out,
            zout, bout, zbuf, bbuf, zf, bf, bias, mbuf, wt, gt, masks, zrelay, brelay,
            zs, bs, fs, zr, br, fr, ms, mr, rs, zrr, brr):
    r, n, c = zin.shape
    passes, hd = wo.shape[0], wo.shape[1]
    heads = wb.shape[1] // 2
    d = hd // heads
    last = passes - 1
    scale = d ** -0.5 * LOG2E

    me_d, me_p = lax.axis_index("data"), lax.axis_index("dap")
    side = math.isqrt(nd)
    cube = side * side == nd and side % 2 == 0 and nm % 4 == 0
    if cube:
        sub = nm // 4
        x, y = me_d // side, me_d % side
        x0, y0 = x - x % 2, y - y % 2
        low = (x % 2) * 2 + y % 2
        mine = me_p // sub
        slot = low * sub + me_p % sub

        def home_of(crop, u):
            return (x0 + crop // 2) * side + y0 + crop % 2, u

        def cube_of(crop, u):
            lo = u // sub
            return (x0 + lo // 2) * side + y0 + lo % 2, crop * sub + u % sub
    else:
        low, mine, slot = me_d, me_d, me_p

        def home_of(crop, u):
            return me_d, u

        cube_of = home_of

    hslot = me_p
    if cube:
        lows = [(low + a) % 4 for a in range(4)]
        places = [(me_p % sub + b) % sub for b in range(sub)]
        lines = [home_of(lo, me_p)[0] for lo in lows]
        stretch = [mine * sub + b for b in places]

    def is_me(t):
        return jnp.logical_and(t[0] == me_d, t[1] == me_p)

    def shifted(base, s):
        return (base + s) % nm

    inside = (low == mine) if cube else True

    def send(src, dst, ss, rs, target, kind, s):
        def local():
            pltpu.make_async_copy(src, dst, rs).start()

        def remote():
            pltpu.make_async_remote_copy(src, dst, ss, rs, device_id=target, device_id_type=MESH).start()

        if kind == "mid" or not cube:
            (local if s == 0 else remote)()
        else:
            me = is_me(target)
            pl.when(me)(local)
            pl.when(jnp.logical_not(me))(remote)

    def drain(ref, sem):
        pltpu.make_async_copy(ref, ref, sem).wait()

    def drain_sent(ref_all, ref_less, sem, kind):
        if kind != "last" or not cube:
            drain(ref_less, sem)
        else:
            pl.when(inside)(lambda: drain(ref_less, sem))
            pl.when(jnp.logical_not(inside))(lambda: drain(ref_all, sem))

    core = me_p % 2

    def hand_on(slot_):
        half = bbuf.at[slot_, :, core]
        drain(half, br.at[slot_])
        pltpu.make_async_remote_copy(half, half, fs, fr.at[slot_], device_id=(me_d, me_p + 1 - 2 * core),
                                     device_id_type=MESH).start()

    def handed_on(slot_):
        half = bbuf.at[slot_, :, core]
        drain(half, fr.at[slot_])
        drain(half, fs)

    barrier = pltpu.get_barrier_semaphore()
    groups = [(home_of, low), (cube_of, mine)] + ([(cube_of, low), (home_of, mine)] if cube else [])
    if not cube:
        groups = groups[:1]
    for of, crop in groups:
        def greet(u, carry, of=of, crop=crop):
            t = of(crop, u)

            @pl.when(jnp.logical_not(is_me(t)))
            def _():
                pl.semaphore_signal(barrier, inc=1, device_id=t, device_id_type=MESH)
            return carry
        lax.fori_loop(0, nm, greet, 0)
    if cube:
        for s in range(1, 4):
            pl.semaphore_signal(barrier, inc=1, device_id=home_of((low + s) % 4, me_p), device_id_type=MESH)

        @pl.when(inside)
        def _():
            pl.semaphore_wait(barrier, 4 * (nm - 1) + 3)

        @pl.when(jnp.logical_not(inside))
        def _():
            pl.semaphore_wait(barrier, 2 * (nm - 1) + 2 * nm + 3)
    else:
        pl.semaphore_wait(barrier, nm - 1)

    low_half = lax.broadcasted_iota(jnp.int32, (2 * heads, LANES), 0) < heads

    def bias_rows(z, w, wbw):
        b = _nt(wbw, _ln(z, w))
        return jnp.where(low_half, b[:, :LANES], b[:, LANES:]).astype(BF16)

    mt = cube_of(low, hslot)
    if cube:
        me_m = is_me(mt)
        pl.when(me_m)(lambda: pltpu.make_async_copy(maskb, mbuf, mr).start())
        pl.when(jnp.logical_not(me_m))(lambda: pltpu.make_async_remote_copy(
            maskb, mbuf, ms, mr, device_id=mt, device_id_type=MESH).start())
    else:
        pltpu.make_async_copy(maskb, mbuf, mr).start()

    def first_bias(i, carry):
        w = small[0]
        for q in range(EDGE_ROWS):
            row = i * EDGE_ROWS + q
            bout[row] = bias_rows(zin[row].astype(F32), w, wb[0])
        return carry
    lax.fori_loop(0, r // EDGE_ROWS, first_bias, 0)
    for s in range(0, nm, 2):
        u = shifted(hslot, s)
        send(bout, bbuf.at[2, hslot // 2, core], bs, br.at[2], home_of(low, u), "mid", s)

    def turn(i, carry):
        gt[i] = jnp.broadcast_to(small[i][2:3], (LANES, hd)).T
        for t, part in enumerate((0, 2, 3)):
            wt[i, t * hd:(t + 1) * hd] = win[i, :, part * hd:(part + 1) * hd].T
        return carry
    lax.fori_loop(0, passes, turn, 0)
    hand_on(2)
    drain(bbuf.at[2, pl.ds(0, nm // 2 - 1), core], bs)
    handed_on(2)
    if cube:
        pl.when(jnp.logical_not(me_m))(lambda: drain(maskb, ms))
    drain(mbuf, mr)
    for k, ref in enumerate((maskb, mbuf)):
        row = ref[...]
        masks[k] = jnp.concatenate([jnp.broadcast_to(row[t:t + 1], (LANES, LANES)).T for t in range(n // LANES)], axis=0)

    def run_pass(p, kind):
        now = 2 if kind == "first" else p % 2
        later = 2 if kind == "last" else (p + 1) % 2
        if kind != "first":
            hand_on(now)
            drain(zbuf.at[now], zr.at[now])

            def widen(i, carry):
                rows = pl.ds(pl.multiple_of(i * r * r, r * r), r * r)
                zf[rows, :] = zbuf[now, pl.ds(i * r, r)].astype(F32).reshape(r * r, c)
                return carry
            lax.fori_loop(0, n // r, widen, 0)
            handed_on(now)

        def widen_bias(i, carry):
            rows = pl.ds(pl.multiple_of(i * r * 2 * heads, r * 2 * heads), r * 2 * heads)
            bf[rows, :] = bbuf[now, i // 2, i % 2].astype(F32).reshape(r * 2 * heads, LANES)
            return carry
        lax.fori_loop(0, n // r, widen_bias, 0)
        mask = masks[0 if kind == "first" else 1]
        for h in range(heads):
            halves = [bf[pl.ds(half * heads + h, n, stride=2 * heads), :] * LOG2E for half in range(2)]
            if kind == "first":
                halves = jnp.split(jnp.concatenate(halves, axis=1).T, 2, axis=1)
            for half in range(2):
                bias[h, :, half * LANES:(half + 1) * LANES] = halves[half] + mask

        crop = low if kind == "first" else mine
        base = hslot if kind == "first" else slot
        of = home_of if kind == "last" else cube_of

        def post(first_row, count, bias_count):
            rows = pl.ds(first_row, count)
            bias_rows_ = pl.ds(first_row + count - bias_count, bias_count)
            for s in range(nm):
                if cube and kind == "mid":
                    u = lows[s // sub] * sub + places[s % sub]
                    target = lines[s // sub], stretch[s % sub]
                else:
                    u = shifted(base, s)
                    target = of(crop, u)
                if kind != "last" and s % 2 == 0 and bias_count:
                    send(bout.at[bias_rows_], bbuf.at[later, base // 2, core, bias_rows_], bs, br.at[later], target, kind, s)
                send(zout.at[rows, pl.ds(pl.multiple_of(u * r, r), r)],
                     zbuf.at[later, pl.ds(base * r + first_row, count)], zs, zr.at[later], target, kind, s)

        def spread(i, count):
            rows = pl.ds(i * count, count)
            for s in range(4):
                lo = (low + s) % 4
                cols = pl.ds(pl.multiple_of(lo * sub * r, r), sub * r)
                target = home_of(lo, me_p)
                send(bout.at[rows], brelay.at[low, rows], rs.at[0], brr.at[i], target, "mid", s)
                send(zout.at[rows, cols], zrelay.at[low, rows], rs.at[1], zrr.at[i], target, "mid", s)

        def relay(i, count):
            rows = pl.ds(i * count, count)
            drain(brelay.at[:, rows], brr.at[i])
            drain(zrelay.at[:, rows], zrr.at[i])
            for s in range(nm):
                u = shifted(me_p, s)
                to = u // sub
                if s % 2 == 0:
                    send(brelay.at[to, rows], bbuf.at[later, me_p // 2, core, rows], bs, br.at[later], (me_d, u), "mid", s)
                cols = pl.ds(pl.multiple_of((u % sub) * r, r), r)
                send(zrelay.at[to, rows, cols], zbuf.at[later, pl.ds(me_p * r + i * count, count)],
                     zs, zr.at[later], (me_d, u), "mid", s)

        def attend(first_row, count, chunks):
            par = small[p]
            w = par[0:2]
            out_b = par[3:4]
            gate_b = jnp.concatenate([gt[p]] * (n // LANES), axis=1)
            zrows, keys, queries, values, gates, raw, outs, news = [], [], [], [], [], [], [], []
            units = [(q, h) for q in range(count) for h in range(heads)]

            def project(q):
                row = first_row + q
                z = zin[row].astype(F32) if kind == "first" else zf[pl.ds(row, n, stride=r), :]
                y = _ln(z, w)
                qvt = _nt(wt[p], y)
                zrows.append(z)
                keys.append(_dot(y, win[p, :, hd:2 * hd]).astype(BF16))
                queries.append(qvt[:hd].astype(BF16))
                values.append(qvt[hd:2 * hd].astype(BF16))
                gates.append(jax.nn.sigmoid(qvt[2 * hd:] + gate_b))

            def scores(q, h):
                parts = [jnp.zeros((d, n), BF16)] * heads
                parts[h] = queries[q][h * d:(h + 1) * d]
                return _dot(keys[q], jnp.concatenate(parts, axis=0))

            def update(q):
                upd = _tn(jnp.concatenate(outs[q * heads:(q + 1) * heads], axis=0), wo[p]) + out_b
                news.append((zrows[q] + upd).astype(BF16))
                zout[first_row + q] = news[q]

            def finish_row(q):
                if kind != "last":
                    bout[first_row + q] = bias_rows(news[q].astype(F32), small[p + 1], wb[p + 1])
                if q + 1 in chunks and not (cube and kind == "first"):
                    since = max((e for e in chunks if e <= q), default=0)
                    whole = (q + 1) % BIAS_ROWS == 0
                    post(first_row + since, q + 1 - since, BIAS_ROWS if whole else 0)

            for q in range(min(AHEAD, count)):
                project(q)
            for j in range(LOOK):
                raw.append(scores(*units[j]))
            for j, (q, h) in enumerate(units):
                if h == 0 and q + AHEAD < count:
                    project(q + AHEAD)
                if j + LOOK < len(units):
                    raw.append(scores(*units[j + LOOK]))
                es, invs = [], []
                for cols in (slice(0, LANES), slice(LANES, 2 * LANES)):
                    sc = raw[j][:, cols] * scale + bias[h, :, cols]
                    e = jnp.exp2(sc - jnp.max(sc, axis=0, keepdims=True))
                    invs.append(1.0 / jnp.sum(e, axis=0, keepdims=True))
                    es.append(e.astype(BF16))
                span = slice(h * d, (h + 1) * d)
                oh = _dot(values[q][span], jnp.concatenate(es, axis=1)) * jnp.concatenate(invs, axis=1)
                outs.append((gates[q][span] * oh).astype(BF16))
                if h == 1 and q > 0:
                    update(q - 1)
                if h == 3 and q > 0:
                    finish_row(q - 1)
            update(count - 1)
            finish_row(count - 1)

        block, chunks = (ROWS, CHUNKS) if kind == "mid" else (EDGE_ROWS, (EDGE_ROWS,))

        def step(i, carry):
            attend(i * block, block, chunks)
            if cube and kind == "first":
                spread(i, block)
                pl.when(i > 0)(lambda: relay(i - 1, block))
            return carry
        lax.fori_loop(0, r // block, step, 0)
        if cube and kind == "first":
            relay(r // block - 1, block)
            drain(zrelay.at[pl.ds(0, 3)], rs.at[1])
            drain(brelay.at[pl.ds(0, 3)], rs.at[0])
        drain_sent(zout, zout.at[:, pl.ds(0, n - r)], zs, kind)
        if kind != "last":
            drain_sent(bbuf.at[now, :, core], bbuf.at[now, pl.ds(0, nm // 2 - 1), core], bs, kind)

    run_pass(0, "first")

    def mid(p, carry):
        run_pass(p, "mid")
        return carry
    lax.fori_loop(1, last, mid, 0)
    run_pass(last, "last")

    end = 2
    drain(zbuf.at[end], zr.at[end])

    def widen(i, carry):
        rows = pl.ds(pl.multiple_of(i * r * r, r * r), r * r)
        zf[rows, :] = zbuf[end, pl.ds(i * r, r)].astype(F32).reshape(r * r, c)
        return carry
    lax.fori_loop(0, n // r, widen, 0)

    def finish(row, carry):
        out[row] = zf[pl.ds(row, n, stride=r), :].astype(BF16)
        return carry
    lax.fori_loop(0, r, finish, 0)


def solution(mesh):
    nd, nm = mesh.shape["data"], mesh.shape["dap"]

    def local(zl, res_mask, ln_w, w_in, b_g, w_b, w_o, b_o):
        r, n, c = zl.shape
        layers, two = w_in.shape[:2]
        m = layers * two
        hd, heads = w_o.shape[2], w_b.shape[3]
        wbt = w_b.reshape(m, c, heads).swapaxes(1, 2)
        wb = jnp.concatenate([wbt, wbt], axis=1)
        small = jnp.concatenate([ln_w, b_g[:, :, None], b_o[:, :, None]], axis=2).astype(F32).reshape(m, 4, c)
        maskb = jnp.where(res_mask > 0, 0.0, NEG * LOG2E).astype(F32).reshape(n // LANES, LANES)
        maskb = jnp.pad(maskb, ((0, 8 - n // LANES), (0, 0)))
        vm = pl.BlockSpec(memory_space=pltpu.VMEM)
        return pl.pallas_call(
            functools.partial(_kernel, nd, nm),
            out_shape=jax.ShapeDtypeStruct((r, n, c), BF16),
            in_specs=[vm] * 6,
            out_specs=vm,
            scratch_shapes=[
                pltpu.VMEM((r, n, c), BF16),
                pltpu.VMEM((r, 2 * heads, LANES), BF16),
                pltpu.VMEM((3, n, r, c), BF16),
                pltpu.VMEM((3, nm // 2, 2, r, 2 * heads, LANES), BF16),
                pltpu.VMEM((n * r, c), F32),
                pltpu.VMEM((n * 2 * heads, LANES), F32),
                pltpu.VMEM((heads, n, n), F32),
                pltpu.VMEM((8, LANES), F32),
                pltpu.VMEM((m, 3 * hd, c), BF16),
                pltpu.VMEM((m, hd, LANES), F32),
                pltpu.VMEM((2, n, LANES), F32),
                pltpu.VMEM((4, r, n // 4, c), BF16),
                pltpu.VMEM((4, r, 2 * heads, LANES), BF16),
                pltpu.SemaphoreType.DMA,
                pltpu.SemaphoreType.DMA,
                pltpu.SemaphoreType.DMA,
                pltpu.SemaphoreType.DMA((3,)),
                pltpu.SemaphoreType.DMA((3,)),
                pltpu.SemaphoreType.DMA((3,)),
                pltpu.SemaphoreType.DMA,
                pltpu.SemaphoreType.DMA,
                pltpu.SemaphoreType.DMA((2,)),
                pltpu.SemaphoreType.DMA((r // EDGE_ROWS,)),
                pltpu.SemaphoreType.DMA((r // EDGE_ROWS,)),
            ],
            compiler_params=pltpu.CompilerParams(collective_id=0, has_side_effects=True, vmem_limit_bytes=56 * 1024 * 1024),
        )(zl, maskb, small, w_in.reshape(m, c, 4 * hd), wb, w_o.reshape(m, hd, c))

    rows = P(('data', 'dap'))
    return jax.shard_map(local, mesh=mesh,
                         in_specs=(rows, P('data'), P(), P(), P(), P(), P(), P()),
                         out_specs=rows, check_vma=False)
```
